256 devices in a mesh: lon: 64 (over x, z_hi, y, core), lat: 4 (over z_lo).
Axes of the slice: x: 4, y: 4, z: 8 (z_hi: 2, z_lo: 4; z = z_hi * 4 + z_lo), core: 2. Of those that a mesh axis runs over, the one named last changes fastest.
Arguments:
- fields: bfloat16 [4, 128, 256, 8192], P(None, None, 'lat', 'lon'), may hold values from -12 to 12
- bracket: int32 [32, 256, 8192], P(None, 'lat', 'lon'), may hold values from 0 to 126, as said below
- fraction: bfloat16 [32, 256, 8192], P(None, 'lat', 'lon'), may hold values from 0 to 1
Outputs:
- on_pressure: bfloat16 [4, 32, 256, 8192], P(None, None, ('lat', 'lon'))
- zonal_mean: float32 [4, 32, 256], P(None, None, ('lat', 'lon'))
- meridional: float32 [4, 32, 256], P(None, None, ('lat', 'lon'))
The draws below stay inside these ranges and needn't reach their ends.
Inputs may be any that keep to these rules, and one draw needn't show every extreme that they name: bracket[p, r, c] - min(p * 4, 112) lies in 0 to 14 for every column, and each of these offsets occurs.
All inputs are finite; a program needn't handle non-finite values.
Results may differ from the reference program's by a relative error of at most 0.0012.
Values may be sent and summed in bfloat16 or wider, within the bound.
A program may use at most 128 MiB of HBM per device.

```python
import jax
import jax.numpy as jnp
from jax import lax

VARS = 4
LEV = 128
PLEV = 32
WINDOW = 16
NLAT = 256
NLON = 8192


def draw_fields(key, part):
    key_noise = jax.random.fold_in(key, 11)
    key_offset = jax.random.fold_in(key, 12)
    noise_part = jnp.clip(jax.random.normal(key_noise, (VARS, LEV, NLAT, NLON), jnp.float32), -4.0, 4.0)
    offset = jax.random.uniform(key_offset, (VARS, LEV, NLAT, 1), jnp.float32, -4.0, 4.0)
    values = noise_part + offset
    return values.astype(jnp.bfloat16)


def draw_bracket(key, part):
    key_offset = jax.random.fold_in(key, 21)
    level_step = LEV // PLEV
    pressure_index = jnp.arange(PLEV, dtype=jnp.int32).reshape(PLEV, 1, 1)
    window_base = jnp.minimum(pressure_index * level_step, LEV - WINDOW)
    offsets = jax.random.randint(key_offset, (PLEV, NLAT, NLON), 0, WINDOW - 1, dtype=jnp.int32)
    return (window_base + offsets).astype(jnp.int32)


def shard_levels(key, shape, cuts, low, largest):
    def one(dim, blocks):
        steps = jax.random.uniform(jax.random.fold_in(jax.random.fold_in(key, 6), dim), (blocks,), jnp.float32, low / len(cuts), largest / len(cuts))
        return jnp.repeat(jnp.exp(steps), shape[dim] // blocks).reshape((-1,) + (1,) * (len(shape) - dim - 1))

    level = one(*cuts[0])
    for cut in cuts[1:]:
        level = level * one(*cut)
    return level


def setup_inputs(seed: int = 0) -> dict:
    streams_of = jax.random.split(jax.random.key(seed), 4)
    return {
        "fields": draw_fields(jax.random.fold_in(streams_of[3], 71), 0),
        "bracket": draw_bracket(jax.random.fold_in(streams_of[3], 71), 0),
        "fraction": jnp.clip(1.0 * jax.random.uniform(streams_of[2], (PLEV, NLAT, NLON), jnp.float32) ** shard_levels(streams_of[2], (PLEV, NLAT, NLON), ((1, 4), (2, 64)), -0.2, 0.2), 0.0, 1.0).astype(jnp.bfloat16),
    }


def interpolate(block, bracket, fraction):
    index = jnp.broadcast_to(bracket[None], (block.shape[0],) + bracket.shape)
    lower_level = jnp.take_along_axis(block, index, axis=1).astype(jnp.float32)
    upper_level = jnp.take_along_axis(block, index + 1, axis=1).astype(jnp.float32)
    weight = fraction.astype(jnp.float32)[None]
    return (lower_level + weight * (upper_level - lower_level)).astype(jnp.bfloat16)


def reference(fields, bracket, fraction):
    on_pressure = lax.map(lambda single: interpolate(single[None], bracket, fraction)[0], fields)
    zonal_mean = jnp.sum(on_pressure.astype(jnp.float32), axis=3) / jnp.float32(NLON)
    centered = 0.5 * (zonal_mean[:, :, 2:] - zonal_mean[:, :, :-2])
    first_row = zonal_mean[:, :, 1:2] - zonal_mean[:, :, 0:1]
    last_row = zonal_mean[:, :, -1:] - zonal_mean[:, :, -2:-1]
    meridional = jnp.concatenate([first_row, centered, last_row], axis=2)
    return on_pressure, zonal_mean, meridional
```

```python
import functools

import jax
import jax.numpy as jnp
from jax import lax
from jax.experimental import pallas as pl
from jax.experimental.pallas import tpu as pltpu
from jax.sharding import Mesh
from jax.sharding import PartitionSpec as P

WINDOW = 16
LON = ("lon_0", "lon_1", "lon_2", "lon_3")
LAT_LON = ("lat", "lon_0", "lon_1", "lon_2", "lon_3")
AXES = ("lon_0", "lon_1", "lon_2", "lon_3", "lat")
MESH_ID = pl.DeviceIdType.MESH
PEERS = 64
GROUPS = 4
ROWS = 16
LANES = 128


def device_of(lon, lat):
    return (lon // 16, (lon // 8) % 2, (lon // 2) % 4, lon % 2, lat)


def kernel(
    fields, bracket, fraction, out, zonal_out, merid_out,
    fbuf, bbuf, wbuf, tbuf, send, zrow, zprev, znext,
    in_sem, send_sem, recv_sem, zsend_sem, zrecv_sem,
):
    nvar = fields.shape[0]
    levels = fields.shape[1]
    plevs = bracket.shape[0]
    step = levels // plevs
    planes = nvar * plevs
    lon_place = (
        (lax.axis_index("lon_0") * 2 + lax.axis_index("lon_1")) * 4 + lax.axis_index("lon_2")
    ) * 2 + lax.axis_index("lon_3")
    lat_place = lax.axis_index("lat")
    row = lat_place * PEERS + lon_place
    next_row = (row + 1) % (4 * PEERS)
    prev_row = (row + 4 * PEERS - 1) % (4 * PEERS)
    next_device = device_of(next_row % PEERS, next_row // PEERS)
    prev_device = device_of(prev_row % PEERS, prev_row // PEERS)

    def group_of(k):
        return (lon_place // ROWS + k) % GROUPS

    def loads(k):
        rows = pl.ds(pl.multiple_of(group_of(k) * ROWS, ROWS), ROWS)
        return (
            pltpu.make_async_copy(fields.at[:, :, rows, :], fbuf.at[k], in_sem.at[k, 0]),
            pltpu.make_async_copy(bracket.at[:, rows, :], bbuf.at[k], in_sem.at[k, 1]),
            pltpu.make_async_copy(fraction.at[:, rows, :], wbuf.at[k], in_sem.at[k, 2]),
        )

    for k in range(GROUPS):
        for copy in loads(k):
            copy.start()

    barrier = pltpu.get_barrier_semaphore()

    def greet(i, carry):
        lon = (lon_place + i) % PEERS
        pl.semaphore_signal(barrier, inc=1, device_id=device_of(lon, lat_place), device_id_type=MESH_ID)
        return carry

    lax.fori_loop(1, PEERS, greet, 0)
    pl.semaphore_signal(barrier, inc=1, device_id=next_device, device_id_type=MESH_ID)
    pl.semaphore_signal(barrier, inc=1, device_id=prev_device, device_id_type=MESH_ID)

    for k in range(GROUPS):
        for copy in loads(k):
            copy.wait()

        def one_level(p, carry, k=k):
            base = jnp.minimum(p * step, levels - WINDOW)
            offset = (bbuf[k, p] - base).astype(jnp.float32).astype(jnp.bfloat16)
            eight = offset >= 8
            offset = jnp.where(eight, offset - 8, offset)
            four = offset >= 4
            offset = jnp.where(four, offset - 4, offset)
            two = offset >= 2
            offset = jnp.where(two, offset - 2, offset)
            one = offset >= 1
            weight = wbuf[k, p].astype(jnp.float32)
            for v in range(nvar):
                w = [fbuf[k, v, base + j] for j in range(WINDOW)]
                w = [jnp.where(eight, w[j + 8], w[j]) for j in range(8)] + [w[8]]
                w = [jnp.where(four, w[j + 4], w[j]) for j in range(5)]
                w = [jnp.where(two, w[j + 2], w[j]) for j in range(3)]
                lower = jnp.where(one, w[1], w[0]).astype(jnp.float32)
                upper = jnp.where(one, w[2], w[1]).astype(jnp.float32)
                value = lower + weight * (upper - lower)
                at = pl.multiple_of((v * plevs + p) * 8, 8)
                tbuf[0, pl.ds(at, 8), :] = value[:8]
                tbuf[1, pl.ds(at, 8), :] = value[8:]
            return carry

        lax.fori_loop(0, plevs, one_level, 0)

        def one_row(r, carry, k=k):
            for half in range(2):
                for q in range(planes // 16):
                    block = tbuf[half, pl.ds(q * 128 + r, 16, stride=8), :]
                    send[k, half * 8 + r, q * 16 : (q + 1) * 16, :] = block.astype(jnp.bfloat16)
            return carry

        lax.fori_loop(0, 8, one_row, 0)

        if k == 0:
            pl.semaphore_wait(barrier, PEERS + 1)
            mine = send[0, lon_place % ROWS]
            out[:, pl.ds(pl.multiple_of(lon_place * LANES, LANES), LANES)] = mine

        def one_send(r, carry, k=k):
            lon = group_of(k) * ROWS + (r + lon_place) % ROWS

            @pl.when(lon != lon_place)
            def _():
                pltpu.make_async_remote_copy(
                    src_ref=send.at[k, lon % ROWS],
                    dst_ref=out.at[:, pl.ds(pl.multiple_of(lon_place * LANES, LANES), LANES)],
                    send_sem=send_sem,
                    recv_sem=recv_sem,
                    device_id=device_of(lon, lat_place),
                    device_id_type=MESH_ID,
                ).start()

            return carry

        lax.fori_loop(0, ROWS, one_send, 0)

    arrived = out.at[:, pl.ds(0, (PEERS - 1) * LANES)]
    pltpu.make_async_copy(arrived, arrived, recv_sem).wait()

    def add_block(i, total):
        block = out[:, pl.ds(pl.multiple_of(i * LANES, LANES), LANES)]
        return total + block.astype(jnp.float32)

    total = lax.fori_loop(0, PEERS, add_block, jnp.zeros((planes, LANES), jnp.float32))
    mean = jnp.sum(total.T, axis=0, keepdims=True) / jnp.float32(PEERS * LANES)
    zrow[...] = jnp.broadcast_to(mean, zrow.shape)

    to_next = pltpu.make_async_remote_copy(
        src_ref=zrow, dst_ref=zprev, send_sem=zsend_sem.at[0], recv_sem=zrecv_sem.at[0],
        device_id=next_device, device_id_type=MESH_ID,
    )
    to_prev = pltpu.make_async_remote_copy(
        src_ref=zrow, dst_ref=znext, send_sem=zsend_sem.at[1], recv_sem=zrecv_sem.at[1],
        device_id=prev_device, device_id_type=MESH_ID,
    )
    to_next.start()
    to_prev.start()
    for v in range(nvar):
        zonal_out[v] = mean[:, v * plevs : (v + 1) * plevs]
    sent = send.at[:, :, pl.ds(0, planes), :]
    all_sent = out.at[:, pl.ds(0, (PEERS - 1) * LANES)]
    pltpu.make_async_copy(all_sent, all_sent, send_sem).wait()
    to_next.wait()
    to_prev.wait()
    above = znext[0:1, :]
    below = zprev[0:1, :]
    slope = jnp.where(
        row == 0,
        above - mean,
        jnp.where(row == 4 * PEERS - 1, mean - below, 0.5 * (above - below)),
    )
    for v in range(nvar):
        merid_out[v] = slope[:, v * plevs : (v + 1) * plevs]


def shards(fields, bracket, fraction):
    nvar, levels, rows, lanes = fields.shape
    plevs = bracket.shape[0]
    planes = nvar * plevs
    hbm = pl.BlockSpec(memory_space=pltpu.MemorySpace.HBM)
    vmem = pl.BlockSpec(memory_space=pltpu.VMEM)
    on_pressure, zonal, merid = pl.pallas_call(
        kernel,
        name="relay",
        out_shape=(
            jax.ShapeDtypeStruct((planes, PEERS * LANES), jnp.bfloat16),
            jax.ShapeDtypeStruct((nvar, 1, plevs), jnp.float32),
            jax.ShapeDtypeStruct((nvar, 1, plevs), jnp.float32),
        ),
        in_specs=[hbm] * 3,
        out_specs=(vmem, vmem, vmem),
        scratch_shapes=[
            pltpu.VMEM((GROUPS, nvar, levels, ROWS, lanes), jnp.bfloat16),
            pltpu.VMEM((GROUPS, plevs, ROWS, lanes), jnp.int32),
            pltpu.VMEM((GROUPS, plevs, ROWS, lanes), jnp.bfloat16),
            pltpu.VMEM((2, planes * 8, lanes), jnp.float32),
            pltpu.VMEM((GROUPS, ROWS, planes, lanes), jnp.bfloat16),
            pltpu.VMEM((8, planes), jnp.float32),
            pltpu.VMEM((8, planes), jnp.float32),
            pltpu.VMEM((8, planes), jnp.float32),
            pltpu.SemaphoreType.DMA((GROUPS, 3)),
            pltpu.SemaphoreType.DMA,
            pltpu.SemaphoreType.DMA,
            pltpu.SemaphoreType.DMA((2,)),
            pltpu.SemaphoreType.DMA((2,)),
        ],
        compiler_params=pltpu.CompilerParams(
            collective_id=0, has_side_effects=True, vmem_limit_bytes=(64 * 1024 - 64 - 2048 - 64) * 1024
        ),
    )(fields, bracket, fraction)
    return (
        on_pressure.reshape(nvar, plevs, 1, PEERS * LANES),
        zonal.transpose(0, 2, 1),
        merid.transpose(0, 2, 1),
    )


def solution(mesh):
    finer = Mesh(
        mesh.devices.reshape(4, 2, 4, 2, mesh.shape["lat"]),
        AXES,
    )
    in_specs = (P(None, None, "lat", LON), P(None, "lat", LON), P(None, "lat", LON))
    out_specs = (P(None, None, LAT_LON, None), P(None, None, LAT_LON), P(None, None, LAT_LON))
    return jax.shard_map(
        shards, mesh=finer, in_specs=in_specs, out_specs=out_specs, check_vma=False
    )
```

```python
import functools

import jax
import jax.numpy as jnp
from jax import lax
from jax.experimental import pallas as pl
from jax.experimental.pallas import tpu as pltpu
from jax.sharding import Mesh
from jax.sharding import PartitionSpec as P

WINDOW = 16
LON = ("lon_0", "lon_1", "lon_2", "lon_3")
LAT_LON = ("lat", "lon_0", "lon_1", "lon_2", "lon_3")
AXES = ("lon_0", "lon_1", "lon_2", "lon_3", "lat")
MESH_ID = pl.DeviceIdType.MESH
PEERS = 64
GROUPS = 4
ROWS = 16
LANES = 128
ROOM_KIB = 15000
PIECES = 2


def device_of(lon, lat):
    return (lon // 16, (lon // 8) % 2, (lon // 2) % 4, lon % 2, lat)


def kernel(
    fields, bracket, fraction, out, zonal_out, merid_out,
    fbuf, bbuf, wbuf, tbuf, send, part, gathered, band, sums,
    in_sem, send_sem, recv_sem, part_send, part_recv, sums_send, sums_recv,
):
    nvar = fields.shape[0]
    levels = fields.shape[1]
    plevs = bracket.shape[0]
    step = levels // plevs
    planes = nvar * plevs
    lon_place = (
        (lax.axis_index("lon_0") * 2 + lax.axis_index("lon_1")) * 4 + lax.axis_index("lon_2")
    ) * 2 + lax.axis_index("lon_3")
    lat_place = lax.axis_index("lat")
    row = lat_place * PEERS + lon_place
    mine_m = lon_place // 8
    mine_j = lon_place % 8

    def group_of(k):
        return (lon_place // ROWS + k) % GROUPS

    def loads(k):
        rows = pl.ds(pl.multiple_of(group_of(k) * ROWS, ROWS), ROWS)
        return (
            pltpu.make_async_copy(fields.at[:, :, rows, :], fbuf.at[k], in_sem.at[k, 0]),
            pltpu.make_async_copy(bracket.at[:, rows, :], bbuf.at[k], in_sem.at[k, 1]),
            pltpu.make_async_copy(fraction.at[:, rows, :], wbuf.at[k], in_sem.at[k, 2]),
        )

    for k in range(GROUPS):
        for copy in loads(k):
            copy.start()

    barrier = pltpu.get_barrier_semaphore()

    def greet(i, carry):
        lon = (lon_place + i) % PEERS
        pl.semaphore_signal(barrier, inc=1, device_id=device_of(lon, lat_place), device_id_type=MESH_ID)
        return carry

    lax.fori_loop(1, PEERS, greet, 0)

    @pl.when(lon_place == 0)
    def _():
        def greet_below(m, carry):
            device = device_of(m * 8 + 7, (lat_place + 3) % 4)
            pl.semaphore_signal(barrier, inc=1, device_id=device, device_id_type=MESH_ID)
            return carry

        lax.fori_loop(0, 8, greet_below, 0)

    @pl.when(lon_place == PEERS - 1)
    def _():
        def greet_above(m, carry):
            device = device_of(m * 8, (lat_place + 1) % 4)
            pl.semaphore_signal(barrier, inc=1, device_id=device, device_id_type=MESH_ID)
            return carry

        lax.fori_loop(0, 8, greet_above, 0)

    ones = jnp.ones((16, LANES), jnp.bfloat16)

    def compute(k):
        for copy in loads(k):
            copy.wait()

        def one_level(p, carry):
            base = jnp.minimum(p * step, levels - WINDOW)
            offset = (bbuf[k, p] - base).astype(jnp.float32).astype(jnp.bfloat16)
            eight = offset >= 8
            offset = jnp.where(eight, offset - 8, offset)
            four = offset >= 4
            offset = jnp.where(four, offset - 4, offset)
            two = offset >= 2
            offset = jnp.where(two, offset - 2, offset)
            one = offset >= 1
            weight = wbuf[k, p].astype(jnp.float32)
            for v in range(nvar):
                w = [fbuf[k, v, base + j] for j in range(WINDOW)]
                w = [jnp.where(eight, w[j + 8], w[j]) for j in range(8)] + [w[8]]
                w = [jnp.where(four, w[j + 4], w[j]) for j in range(5)]
                w = [jnp.where(two, w[j + 2], w[j]) for j in range(3)]
                lower = jnp.where(one, w[1], w[0]).astype(jnp.float32)
                upper = jnp.where(one, w[2], w[1]).astype(jnp.float32)
                value = lower + weight * (upper - lower)
                at = pl.multiple_of((v * plevs + p) * 8, 8)
                tbuf[0, pl.ds(at, 8), :] = value[:8]
                tbuf[1, pl.ds(at, 8), :] = value[8:]
            return carry

        lax.fori_loop(0, plevs, one_level, 0)

        def one_row(r, carry):
            for half in range(2):
                for q in range(planes // 16):
                    block = tbuf[half, pl.ds(q * 128 + r, 16, stride=8), :]
                    send[k, half * 8 + r, q * 16 : (q + 1) * 16, :] = block.astype(jnp.bfloat16)
            for half in range(2):
                total = lax.dot_general(
                    ones, send[k, half * 8 + r], (((1,), (1,)), ((), ())),
                    preferred_element_type=jnp.float32,
                )
                part[r, group_of(k) * 2 + half] = total[0:1]
            return carry

        lax.fori_loop(0, 8, one_row, 0)

    def send_group(k):
        def one_send(r, carry):
            lon = group_of(k) * ROWS + (r + (mine_m + 1) % 2 * 8) % ROWS

            @pl.when(lon != lon_place)
            def _():
                pltpu.make_async_remote_copy(
                    src_ref=send.at[k, lon % ROWS],
                    dst_ref=out.at[:, pl.ds(pl.multiple_of(lon_place * LANES, LANES), LANES)],
                    send_sem=send_sem,
                    recv_sem=recv_sem,
                    device_id=device_of(lon, lat_place),
                    device_id_type=MESH_ID,
                ).start()

            return carry

        lax.fori_loop(0, ROWS, one_send, 0)

    compute(0)
    out[:, pl.ds(pl.multiple_of(lon_place * LANES, LANES), LANES)] = send[0, lon_place % ROWS]
    pl.semaphore_wait(
        barrier,
        PEERS - 1 + (mine_j == 0).astype(jnp.int32) + (mine_j == 7).astype(jnp.int32),
    )
    send_group(0)
    for k in range(1, GROUPS):
        compute(k)

    def send_part(i, carry):
        j = (mine_j + i) % 8
        pltpu.make_async_remote_copy(
            src_ref=part.at[j],
            dst_ref=gathered.at[mine_j],
            send_sem=part_send,
            recv_sem=part_recv,
            device_id=device_of(mine_m * 8 + j, lat_place),
            device_id_type=MESH_ID,
        ).start()
        return carry

    lax.fori_loop(1, 8, send_part, 0)
    gathered[mine_j] = part[mine_j]
    send_group(1)
    seven = gathered.at[pl.ds(0, 7)]
    pltpu.make_async_copy(seven, seven, part_recv).wait()
    subtotal = gathered[0]
    for j in range(1, 8):
        subtotal = subtotal + gathered[j]
    band[...] = subtotal

    def send_sums(m, carry):
        here = lat_place * PEERS + m * 8 + mine_j
        for shift in (-1, 0, 1):
            there = (here + shift + 4 * PEERS) % (4 * PEERS)

            @pl.when(there != row)
            def _(shift=shift, there=there):
                pltpu.make_async_remote_copy(
                    src_ref=band.at[m],
                    dst_ref=sums.at[(1 - shift) * 8 + mine_m],
                    send_sem=sums_send,
                    recv_sem=sums_recv,
                    device_id=device_of(there % PEERS, there // PEERS),
                    device_id_type=MESH_ID,
                ).start()

        return carry

    lax.fori_loop(0, 8, send_sums, 0)
    sums[8 + mine_m] = band[mine_m]
    for k in range(2, GROUPS):
        send_group(k)

    most = sums.at[pl.ds(0, 23)]
    pltpu.make_async_copy(most, most, sums_recv).wait()
    means = []
    for slot in range(3):
        total = sums[slot * 8]
        for m in range(1, 8):
            total = total + sums[slot * 8 + m]
        means.append(total / jnp.float32(PEERS * LANES))
    below, mean, above = means
    slope = jnp.where(
        row == 0,
        above - mean,
        jnp.where(row == 4 * PEERS - 1, mean - below, 0.5 * (above - below)),
    )
    for v in range(nvar):
        zonal_out[v] = mean[:, v * plevs : (v + 1) * plevs]
        merid_out[v] = slope[:, v * plevs : (v + 1) * plevs]
    pltpu.make_async_copy(seven, seven, part_send).wait()
    pltpu.make_async_copy(most, most, sums_send).wait()
    arrived = out.at[:, pl.ds(0, (PEERS - 1) * LANES)]
    pltpu.make_async_copy(arrived, arrived, send_sem).wait()
    pltpu.make_async_copy(arrived, arrived, recv_sem).wait()


def finish(relaid, zonal, merid, out, zonal_out, merid_out, sem):
    copies = [
        pltpu.make_async_copy(zonal, zonal_out, sem.at[0]),
        pltpu.make_async_copy(merid, merid_out, sem.at[1]),
    ]
    for i in range(PIECES):
        rows = pl.ds(i * relaid.shape[0] // PIECES, relaid.shape[0] // PIECES)
        copies.append(pltpu.make_async_copy(relaid.at[rows], out.at[rows], sem.at[i + 2]))
    for copy in copies:
        copy.start()
    for copy in copies:
        copy.wait()


def shards(fields, bracket, fraction):
    nvar, levels, rows, lanes = fields.shape
    plevs = bracket.shape[0]
    planes = nvar * plevs
    hbm = pl.BlockSpec(memory_space=pltpu.MemorySpace.HBM)
    vmem = pl.BlockSpec(memory_space=pltpu.VMEM)
    args = [
        pltpu.with_memory_space_constraint(x, pltpu.MemorySpace.HBM)
        for x in (fields, bracket, fraction)
    ]
    on_pressure, zonal, merid = pl.pallas_call(
        kernel,
        name="relay",
        out_shape=(
            jax.ShapeDtypeStruct((planes, PEERS * LANES), jnp.bfloat16),
            jax.ShapeDtypeStruct((nvar, 1, plevs), jnp.float32),
            jax.ShapeDtypeStruct((nvar, 1, plevs), jnp.float32),
        ),
        in_specs=[hbm] * 3,
        out_specs=(vmem, vmem, vmem),
        scratch_shapes=[
            pltpu.VMEM((GROUPS, nvar, levels, ROWS, lanes), jnp.bfloat16),
            pltpu.VMEM((GROUPS, plevs, ROWS, lanes), jnp.int32),
            pltpu.VMEM((GROUPS, plevs, ROWS, lanes), jnp.bfloat16),
            pltpu.VMEM((2, planes * 8, lanes), jnp.float32),
            pltpu.VMEM((GROUPS, ROWS, planes, lanes), jnp.bfloat16),
            pltpu.VMEM((8, 8, 1, planes), jnp.float32),
            pltpu.VMEM((8, 8, 1, planes), jnp.float32),
            pltpu.VMEM((8, 1, planes), jnp.float32),
            pltpu.VMEM((24, 1, planes), jnp.float32),
            pltpu.SemaphoreType.DMA((GROUPS, 3)),
            pltpu.SemaphoreType.DMA,
            pltpu.SemaphoreType.DMA,
            pltpu.SemaphoreType.DMA,
            pltpu.SemaphoreType.DMA,
            pltpu.SemaphoreType.DMA,
            pltpu.SemaphoreType.DMA,
        ],
        compiler_params=pltpu.CompilerParams(
            collective_id=0, has_side_effects=True, vmem_limit_bytes=(64 * 1024 - ROOM_KIB) * 1024
        ),
    )(*args)
    on_pressure, zonal, merid = pl.pallas_call(
        finish,
        name="finish",
        out_shape=(
            jax.ShapeDtypeStruct((planes, PEERS * LANES), jnp.bfloat16),
            jax.ShapeDtypeStruct((nvar, 1, plevs), jnp.float32),
            jax.ShapeDtypeStruct((nvar, 1, plevs), jnp.float32),
        ),
        in_specs=[pl.BlockSpec(memory_space=pl.ANY)] * 3,
        out_specs=(hbm, hbm, hbm),
        scratch_shapes=[pltpu.SemaphoreType.DMA((PIECES + 2,))],
        compiler_params=pltpu.CompilerParams(vmem_limit_bytes=1 * 2**20),
    )(on_pressure, zonal, merid)
    return (
        on_pressure.reshape(nvar, plevs, 1, PEERS * LANES),
        zonal.transpose(0, 2, 1),
        merid.transpose(0, 2, 1),
    )


def solution(mesh):
    finer = Mesh(
        mesh.devices.reshape(4, 2, 4, 2, mesh.shape["lat"]),
        AXES,
    )
    in_specs = (P(None, None, "lat", LON), P(None, "lat", LON), P(None, "lat", LON))
    out_specs = (P(None, None, LAT_LON, None), P(None, None, LAT_LON), P(None, None, LAT_LON))
    return jax.shard_map(
        shards, mesh=finer, in_specs=in_specs, out_specs=out_specs, check_vma=False
    )
```

```python
import functools

import jax
import jax.numpy as jnp
from jax import lax
from jax.experimental import pallas as pl
from jax.experimental.pallas import tpu as pltpu
from jax.sharding import Mesh
from jax.sharding import PartitionSpec as P

WINDOW = 16
LON = ("lon_0", "lon_1", "lon_2", "lon_3")
LAT_LON = ("lat", "lon_0", "lon_1", "lon_2", "lon_3")
AXES = ("lon_0", "lon_1", "lon_2", "lon_3", "lat")
MESH_ID = pl.DeviceIdType.MESH
PEERS = 64
GROUPS = 4
ROWS = 16
LANES = 128
ROOM_KIB = 15000
PIECES = 2
X_ORDER = (1, 3, 2, 0)


def device_of(lon, lat):
    return (lon // 16, (lon // 8) % 2, (lon // 2) % 4, lon % 2, lat)


def kernel(
    fields, bracket, fraction, out, zonal_out, merid_out,
    fbuf, bbuf, wbuf, tbuf, send, part, gathered, band, sums,
    in_sem, send_sem, recv_sem, part_send, part_recv, sums_send, sums_recv,
):
    nvar = fields.shape[0]
    levels = fields.shape[1]
    plevs = bracket.shape[0]
    step = levels // plevs
    planes = nvar * plevs
    lon_place = (
        (lax.axis_index("lon_0") * 2 + lax.axis_index("lon_1")) * 4 + lax.axis_index("lon_2")
    ) * 2 + lax.axis_index("lon_3")
    lat_place = lax.axis_index("lat")
    row = lat_place * PEERS + lon_place
    mine_m = lon_place // 8
    mine_j = lon_place % 8

    def group_of(k):
        return (lon_place // ROWS + X_ORDER[k]) % GROUPS

    def loads(k):
        rows = pl.ds(pl.multiple_of(group_of(k) * ROWS, ROWS), ROWS)
        return (
            pltpu.make_async_copy(fields.at[:, :, rows, :], fbuf.at[k], in_sem.at[k, 0]),
            pltpu.make_async_copy(bracket.at[:, rows, :], bbuf.at[k], in_sem.at[k, 1]),
            pltpu.make_async_copy(fraction.at[:, rows, :], wbuf.at[k], in_sem.at[k, 2]),
        )

    for k in range(GROUPS):
        for copy in loads(k):
            copy.start()

    barrier = pltpu.get_barrier_semaphore()

    def greet(i, carry):
        lon = (lon_place + i) % PEERS
        pl.semaphore_signal(barrier, inc=1, device_id=device_of(lon, lat_place), device_id_type=MESH_ID)
        return carry

    lax.fori_loop(1, PEERS, greet, 0)

    @pl.when(lon_place == 0)
    def _():
        def greet_below(m, carry):
            device = device_of(m * 8 + 7, (lat_place + 3) % 4)
            pl.semaphore_signal(barrier, inc=1, device_id=device, device_id_type=MESH_ID)
            return carry

        lax.fori_loop(0, 8, greet_below, 0)

    @pl.when(lon_place == PEERS - 1)
    def _():
        def greet_above(m, carry):
            device = device_of(m * 8, (lat_place + 1) % 4)
            pl.semaphore_signal(barrier, inc=1, device_id=device, device_id_type=MESH_ID)
            return carry

        lax.fori_loop(0, 8, greet_above, 0)

    ones = jnp.ones((16, LANES), jnp.bfloat16)

    def compute(k):
        for copy in loads(k):
            copy.wait()

        def one_level(p, carry):
            base = jnp.minimum(p * step, levels - WINDOW)
            offset = (bbuf[k, p] - base).astype(jnp.float32).astype(jnp.bfloat16)
            eight = offset >= 8
            offset = jnp.where(eight, offset - 8, offset)
            four = offset >= 4
            offset = jnp.where(four, offset - 4, offset)
            two = offset >= 2
            offset = jnp.where(two, offset - 2, offset)
            one = offset >= 1
            weight = wbuf[k, p].astype(jnp.float32)
            for v in range(nvar):
                w = [fbuf[k, v, base + j] for j in range(WINDOW)]
                w = [jnp.where(eight, w[j + 8], w[j]) for j in range(8)] + [w[8]]
                w = [jnp.where(four, w[j + 4], w[j]) for j in range(5)]
                w = [jnp.where(two, w[j + 2], w[j]) for j in range(3)]
                lower = jnp.where(one, w[1], w[0]).astype(jnp.float32)
                upper = jnp.where(one, w[2], w[1]).astype(jnp.float32)
                value = lower + weight * (upper - lower)
                at = pl.multiple_of((v * plevs + p) * 8, 8)
                tbuf[0, pl.ds(at, 8), :] = value[:8]
                tbuf[1, pl.ds(at, 8), :] = value[8:]
            return carry

        lax.fori_loop(0, plevs, one_level, 0)

        def one_row(r, carry):
            for half in range(2):
                for q in range(planes // 16):
                    block = tbuf[half, pl.ds(q * 128 + r, 16, stride=8), :]
                    send[k, half * 8 + r, q * 16 : (q + 1) * 16, :] = block.astype(jnp.bfloat16)
            for half in range(2):
                total = lax.dot_general(
                    ones, send[k, half * 8 + r], (((1,), (1,)), ((), ())),
                    preferred_element_type=jnp.float32,
                )
                part[r, group_of(k) * 2 + half] = total[0:1]
            return carry

        lax.fori_loop(0, 8, one_row, 0)

    place_y = (lon_place // 2) % 4
    place_c = lon_place % 2
    place_zh = mine_m % 2

    def send_half(k, cross):
        def one_send(i, carry):
            y = (place_y + 1 + i // 2) % 4
            c = (place_c + i) % 2
            half = (place_zh + cross) % 2
            lon = group_of(k) * ROWS + half * 8 + y * 2 + c

            @pl.when(lon != lon_place)
            def _():
                pltpu.make_async_remote_copy(
                    src_ref=send.at[k, lon % ROWS],
                    dst_ref=out.at[:, pl.ds(pl.multiple_of(lon_place * LANES, LANES), LANES)],
                    send_sem=send_sem,
                    recv_sem=recv_sem,
                    device_id=device_of(lon, lat_place),
                    device_id_type=MESH_ID,
                ).start()

            return carry

        lax.fori_loop(0, 8, one_send, 0)

    def send_group(k):
        send_half(k, 1)
        send_half(k, 0)

    compute(0)
    pl.semaphore_wait(
        barrier,
        PEERS - 1 + (mine_j == 0).astype(jnp.int32) + (mine_j == 7).astype(jnp.int32),
    )
    send_half(0, 1)
    for k in range(1, GROUPS):
        compute(k)
    mine = send[X_ORDER.index(0), lon_place % ROWS]
    out[:, pl.ds(pl.multiple_of(lon_place * LANES, LANES), LANES)] = mine

    def send_part(i, carry):
        j = (mine_j + i) % 8
        pltpu.make_async_remote_copy(
            src_ref=part.at[j],
            dst_ref=gathered.at[mine_j],
            send_sem=part_send,
            recv_sem=part_recv,
            device_id=device_of(mine_m * 8 + j, lat_place),
            device_id_type=MESH_ID,
        ).start()
        return carry

    lax.fori_loop(1, 8, send_part, 0)
    gathered[mine_j] = part[mine_j]
    send_half(1, 1)
    seven = gathered.at[pl.ds(0, 7)]
    pltpu.make_async_copy(seven, seven, part_recv).wait()
    subtotal = gathered[0]
    for j in range(1, 8):
        subtotal = subtotal + gathered[j]
    band[...] = subtotal

    def send_sums(m, carry):
        here = lat_place * PEERS + m * 8 + mine_j
        for shift in (-1, 0, 1):
            there = (here + shift + 4 * PEERS) % (4 * PEERS)

            @pl.when(there != row)
            def _(shift=shift, there=there):
                pltpu.make_async_remote_copy(
                    src_ref=band.at[m],
                    dst_ref=sums.at[(1 - shift) * 8 + mine_m],
                    send_sem=sums_send,
                    recv_sem=sums_recv,
                    device_id=device_of(there % PEERS, there // PEERS),
                    device_id_type=MESH_ID,
                ).start()

        return carry

    lax.fori_loop(0, 8, send_sums, 0)
    sums[8 + mine_m] = band[mine_m]
    for k in range(2, GROUPS):
        send_half(k, 1)
    for k in range(GROUPS):
        send_half(k, 0)

    most = sums.at[pl.ds(0, 23)]
    pltpu.make_async_copy(most, most, sums_recv).wait()
    means = []
    for slot in range(3):
        total = sums[slot * 8]
        for m in range(1, 8):
            total = total + sums[slot * 8 + m]
        means.append(total / jnp.float32(PEERS * LANES))
    below, mean, above = means
    slope = jnp.where(
        row == 0,
        above - mean,
        jnp.where(row == 4 * PEERS - 1, mean - below, 0.5 * (above - below)),
    )
    for v in range(nvar):
        zonal_out[v] = mean[:, v * plevs : (v + 1) * plevs]
        merid_out[v] = slope[:, v * plevs : (v + 1) * plevs]
    pltpu.make_async_copy(seven, seven, part_send).wait()
    pltpu.make_async_copy(most, most, sums_send).wait()
    arrived = out.at[:, pl.ds(0, (PEERS - 1) * LANES)]
    pltpu.make_async_copy(arrived, arrived, send_sem).wait()
    pltpu.make_async_copy(arrived, arrived, recv_sem).wait()


def finish(relaid, zonal, merid, out, zonal_out, merid_out, sem):
    copies = [
        pltpu.make_async_copy(zonal, zonal_out, sem.at[0]),
        pltpu.make_async_copy(merid, merid_out, sem.at[1]),
    ]
    for i in range(PIECES):
        rows = pl.ds(i * relaid.shape[0] // PIECES, relaid.shape[0] // PIECES)
        copies.append(pltpu.make_async_copy(relaid.at[rows], out.at[rows], sem.at[i + 2]))
    for copy in copies:
        copy.start()
    for copy in copies:
        copy.wait()


def shards(fields, bracket, fraction):
    nvar, levels, rows, lanes = fields.shape
    plevs = bracket.shape[0]
    planes = nvar * plevs
    hbm = pl.BlockSpec(memory_space=pltpu.MemorySpace.HBM)
    vmem = pl.BlockSpec(memory_space=pltpu.VMEM)
    args = [
        pltpu.with_memory_space_constraint(x, pltpu.MemorySpace.HBM)
        for x in (fields, bracket, fraction)
    ]
    on_pressure, zonal, merid = pl.pallas_call(
        kernel,
        name="relay",
        out_shape=(
            jax.ShapeDtypeStruct((planes, PEERS * LANES), jnp.bfloat16),
            jax.ShapeDtypeStruct((nvar, 1, plevs), jnp.float32),
            jax.ShapeDtypeStruct((nvar, 1, plevs), jnp.float32),
        ),
        in_specs=[hbm] * 3,
        out_specs=(vmem, vmem, vmem),
        scratch_shapes=[
            pltpu.VMEM((GROUPS, nvar, levels, ROWS, lanes), jnp.bfloat16),
            pltpu.VMEM((GROUPS, plevs, ROWS, lanes), jnp.int32),
            pltpu.VMEM((GROUPS, plevs, ROWS, lanes), jnp.bfloat16),
            pltpu.VMEM((2, planes * 8, lanes), jnp.float32),
            pltpu.VMEM((GROUPS, ROWS, planes, lanes), jnp.bfloat16),
            pltpu.VMEM((8, 8, 1, planes), jnp.float32),
            pltpu.VMEM((8, 8, 1, planes), jnp.float32),
            pltpu.VMEM((8, 1, planes), jnp.float32),
            pltpu.VMEM((24, 1, planes), jnp.float32),
            pltpu.SemaphoreType.DMA((GROUPS, 3)),
            pltpu.SemaphoreType.DMA,
            pltpu.SemaphoreType.DMA,
            pltpu.SemaphoreType.DMA,
            pltpu.SemaphoreType.DMA,
            pltpu.SemaphoreType.DMA,
            pltpu.SemaphoreType.DMA,
        ],
        compiler_params=pltpu.CompilerParams(
            collective_id=0, has_side_effects=True, vmem_limit_bytes=(64 * 1024 - ROOM_KIB) * 1024
        ),
    )(*args)
    on_pressure, zonal, merid = pl.pallas_call(
        finish,
        name="finish",
        out_shape=(
            jax.ShapeDtypeStruct((planes, PEERS * LANES), jnp.bfloat16),
            jax.ShapeDtypeStruct((nvar, 1, plevs), jnp.float32),
            jax.ShapeDtypeStruct((nvar, 1, plevs), jnp.float32),
        ),
        in_specs=[pl.BlockSpec(memory_space=pl.ANY)] * 3,
        out_specs=(hbm, hbm, hbm),
        scratch_shapes=[pltpu.SemaphoreType.DMA((PIECES + 2,))],
        compiler_params=pltpu.CompilerParams(vmem_limit_bytes=1 * 2**20),
    )(on_pressure, zonal, merid)
    return (
        on_pressure.reshape(nvar, plevs, 1, PEERS * LANES),
        zonal.transpose(0, 2, 1),
        merid.transpose(0, 2, 1),
    )


def solution(mesh):
    finer = Mesh(
        mesh.devices.reshape(4, 2, 4, 2, mesh.shape["lat"]),
        AXES,
    )
    in_specs = (P(None, None, "lat", LON), P(None, "lat", LON), P(None, "lat", LON))
    out_specs = (P(None, None, LAT_LON, None), P(None, None, LAT_LON), P(None, None, LAT_LON))
    return jax.shard_map(
        shards, mesh=finer, in_specs=in_specs, out_specs=out_specs, check_vma=False
    )
```

```python
import functools

import jax
import jax.numpy as jnp
from jax import lax
from jax.experimental import pallas as pl
from jax.experimental.pallas import tpu as pltpu
from jax.sharding import Mesh
from jax.sharding import PartitionSpec as P

WINDOW = 16
LON = ("lon_0", "lon_1", "lon_2", "lon_3")
LAT_LON = ("lat", "lon_0", "lon_1", "lon_2", "lon_3")
AXES = ("lon_0", "lon_1", "lon_2", "lon_3", "lat")
MESH_ID = pl.DeviceIdType.MESH
PEERS = 64
GROUPS = 4
ROWS = 16
LANES = 128
ROOM_KIB = 15000
PIECES = 2
X_ORDER = (1, 3, 2, 0)


def device_of(lon, lat):
    return (lon // 16, (lon // 8) % 2, (lon // 2) % 4, lon % 2, lat)


def kernel(
    fields, bracket, fraction, out, zonal_out, merid_out,
    fbuf, bbuf, wbuf, tbuf, send, part, gathered, band, sums,
    in_sem, send_sem, recv_sem, part_send, part_recv, sums_send, sums_recv,
):
    nvar = fields.shape[0]
    levels = fields.shape[1]
    plevs = bracket.shape[0]
    step = levels // plevs
    planes = nvar * plevs
    lon_place = (
        (lax.axis_index("lon_0") * 2 + lax.axis_index("lon_1")) * 4 + lax.axis_index("lon_2")
    ) * 2 + lax.axis_index("lon_3")
    lat_place = lax.axis_index("lat")
    row = lat_place * PEERS + lon_place
    mine_m = lon_place // 8
    mine_j = lon_place % 8

    def group_of(k):
        return (lon_place // ROWS + GROUPS + (1 - 2 * (lon_place % 2)) * X_ORDER[k]) % GROUPS

    def loads(k):
        rows = pl.ds(pl.multiple_of(group_of(k) * ROWS, ROWS), ROWS)
        return (
            pltpu.make_async_copy(fields.at[:, :, rows, :], fbuf.at[k], in_sem.at[k, 0]),
            pltpu.make_async_copy(bracket.at[:, rows, :], bbuf.at[k], in_sem.at[k, 1]),
            pltpu.make_async_copy(fraction.at[:, rows, :], wbuf.at[k], in_sem.at[k, 2]),
        )

    for copy in loads(0):
        copy.start()

    barrier = pltpu.get_barrier_semaphore()

    def greet(i, carry):
        lon = (lon_place + i) % PEERS
        pl.semaphore_signal(barrier, inc=1, device_id=device_of(lon, lat_place), device_id_type=MESH_ID)
        return carry

    lax.fori_loop(1, PEERS, greet, 0)

    @pl.when(lon_place == 0)
    def _():
        def greet_below(m, carry):
            device = device_of(m * 8 + 7, (lat_place + 3) % 4)
            pl.semaphore_signal(barrier, inc=1, device_id=device, device_id_type=MESH_ID)
            return carry

        lax.fori_loop(0, 8, greet_below, 0)

    @pl.when(lon_place == PEERS - 1)
    def _():
        def greet_above(m, carry):
            device = device_of(m * 8, (lat_place + 1) % 4)
            pl.semaphore_signal(barrier, inc=1, device_id=device, device_id_type=MESH_ID)
            return carry

        lax.fori_loop(0, 8, greet_above, 0)

    ones = jnp.ones((16, LANES), jnp.bfloat16)

    def compute(k):
        for copy in loads(k):
            copy.wait()
        if k + 1 < GROUPS:
            for copy in loads(k + 1):
                copy.start()

        def one_level(p, carry):
            base = jnp.minimum(p * step, levels - WINDOW)
            offset = (bbuf[k, p] - base).astype(jnp.float32).astype(jnp.bfloat16)
            eight = offset >= 8
            offset = jnp.where(eight, offset - 8, offset)
            four = offset >= 4
            offset = jnp.where(four, offset - 4, offset)
            two = offset >= 2
            offset = jnp.where(two, offset - 2, offset)
            one = offset >= 1
            weight = wbuf[k, p].astype(jnp.float32)
            for v in range(nvar):
                w = [fbuf[k, v, base + j] for j in range(WINDOW)]
                w = [jnp.where(eight, w[j + 8], w[j]) for j in range(8)] + [w[8]]
                w = [jnp.where(four, w[j + 4], w[j]) for j in range(5)]
                w = [jnp.where(two, w[j + 2], w[j]) for j in range(3)]
                lower = jnp.where(one, w[1], w[0]).astype(jnp.float32)
                upper = jnp.where(one, w[2], w[1]).astype(jnp.float32)
                value = lower + weight * (upper - lower)
                at = pl.multiple_of((v * plevs + p) * 8, 8)
                tbuf[0, pl.ds(at, 8), :] = value[:8]
                tbuf[1, pl.ds(at, 8), :] = value[8:]
            return carry

        lax.fori_loop(0, plevs, one_level, 0)

        def one_row(r, carry):
            for half in range(2):
                for q in range(planes // 16):
                    block = tbuf[half, pl.ds(q * 128 + r, 16, stride=8), :]
                    send[k, half * 8 + r, q * 16 : (q + 1) * 16, :] = block.astype(jnp.bfloat16)
            for half in range(2):
                total = lax.dot_general(
                    ones, send[k, half * 8 + r], (((1,), (1,)), ((), ())),
                    preferred_element_type=jnp.float32,
                )
                part[r, group_of(k) * 2 + half] = total[0:1]
            return carry

        lax.fori_loop(0, 8, one_row, 0)

    place_y = (lon_place // 2) % 4
    place_c = lon_place % 2
    place_zh = mine_m % 2

    def send_half(k, cross):
        def one_send(i, carry):
            y = (place_y + 1 + i // 2) % 4
            c = (place_c + i) % 2
            half = (place_zh + cross) % 2
            lon = group_of(k) * ROWS + half * 8 + y * 2 + c

            @pl.when(lon != lon_place)
            def _():
                pltpu.make_async_remote_copy(
                    src_ref=send.at[k, lon % ROWS],
                    dst_ref=out.at[:, pl.ds(pl.multiple_of(lon_place * LANES, LANES), LANES)],
                    send_sem=send_sem.at[k, cross],
                    recv_sem=recv_sem,
                    device_id=device_of(lon, lat_place),
                    device_id_type=MESH_ID,
                ).start()

            return carry

        lax.fori_loop(0, 8, one_send, 0)

    def wait_sent(k, cross):
        count = 7 if X_ORDER[k] == 0 and cross == 0 else 8
        blocks = send.at[k, pl.ds(0, count)]
        pltpu.make_async_copy(blocks, blocks, send_sem.at[k, cross]).wait()

    def send_part(i, carry):
        j = (mine_j + i) % 8
        pltpu.make_async_remote_copy(
            src_ref=part.at[j],
            dst_ref=gathered.at[mine_j],
            send_sem=part_send,
            recv_sem=part_recv,
            device_id=device_of(mine_m * 8 + j, lat_place),
            device_id_type=MESH_ID,
        ).start()
        return carry

    compute(0)
    pl.semaphore_wait(
        barrier,
        PEERS - 1 + (mine_j == 0).astype(jnp.int32) + (mine_j == 7).astype(jnp.int32),
    )
    send_half(0, 1)
    compute(1)
    compute(2)
    compute(3)
    mine = send[X_ORDER.index(0), lon_place % ROWS]
    out[:, pl.ds(pl.multiple_of(lon_place * LANES, LANES), LANES)] = mine
    lax.fori_loop(1, 8, send_part, 0)
    gathered[mine_j] = part[mine_j]
    send_half(1, 1)
    seven = gathered.at[pl.ds(0, 7)]
    pltpu.make_async_copy(seven, seven, part_recv).wait()
    subtotal = gathered[0]
    for j in range(1, 8):
        subtotal = subtotal + gathered[j]
    band[...] = subtotal

    def send_sums(m, carry):
        here = lat_place * PEERS + m * 8 + mine_j
        for shift in (-1, 0, 1):
            there = (here + shift + 4 * PEERS) % (4 * PEERS)

            @pl.when(there != row)
            def _(shift=shift, there=there):
                pltpu.make_async_remote_copy(
                    src_ref=band.at[m],
                    dst_ref=sums.at[(1 - shift) * 8 + mine_m],
                    send_sem=sums_send,
                    recv_sem=sums_recv,
                    device_id=device_of(there % PEERS, there // PEERS),
                    device_id_type=MESH_ID,
                ).start()

        return carry

    lax.fori_loop(0, 8, send_sums, 0)
    sums[8 + mine_m] = band[mine_m]
    send_half(2, 1)
    send_half(3, 1)
    for k in range(GROUPS):
        send_half(k, 0)
    most = sums.at[pl.ds(0, 23)]
    pltpu.make_async_copy(most, most, sums_recv).wait()
    means = []
    for slot in range(3):
        total = sums[slot * 8]
        for m in range(1, 8):
            total = total + sums[slot * 8 + m]
        means.append(total / jnp.float32(PEERS * LANES))
    below, mean, above = means
    slope = jnp.where(
        row == 0,
        above - mean,
        jnp.where(row == 4 * PEERS - 1, mean - below, 0.5 * (above - below)),
    )
    for v in range(nvar):
        zonal_out[v] = mean[:, v * plevs : (v + 1) * plevs]
        merid_out[v] = slope[:, v * plevs : (v + 1) * plevs]
    pltpu.make_async_copy(seven, seven, part_send).wait()
    pltpu.make_async_copy(most, most, sums_send).wait()
    for k in range(GROUPS):
        wait_sent(k, 1)
        wait_sent(k, 0)
    arrived = out.at[:, pl.ds(0, (PEERS - 1) * LANES)]
    pltpu.make_async_copy(arrived, arrived, recv_sem).wait()


def finish(relaid, zonal, merid, out, zonal_out, merid_out, sem):
    copies = [
        pltpu.make_async_copy(zonal, zonal_out, sem.at[0]),
        pltpu.make_async_copy(merid, merid_out, sem.at[1]),
    ]
    for i in range(PIECES):
        rows = pl.ds(i * relaid.shape[0] // PIECES, relaid.shape[0] // PIECES)
        copies.append(pltpu.make_async_copy(relaid.at[rows], out.at[rows], sem.at[i + 2]))
    for copy in copies:
        copy.start()
    for copy in copies:
        copy.wait()


def shards(fields, bracket, fraction):
    nvar, levels, rows, lanes = fields.shape
    plevs = bracket.shape[0]
    planes = nvar * plevs
    hbm = pl.BlockSpec(memory_space=pltpu.MemorySpace.HBM)
    vmem = pl.BlockSpec(memory_space=pltpu.VMEM)
    args = [
        pltpu.with_memory_space_constraint(x, pltpu.MemorySpace.HBM)
        for x in (fields, bracket, fraction)
    ]
    on_pressure, zonal, merid = pl.pallas_call(
        kernel,
        name="relay",
        out_shape=(
            jax.ShapeDtypeStruct((planes, PEERS * LANES), jnp.bfloat16),
            jax.ShapeDtypeStruct((nvar, 1, plevs), jnp.float32),
            jax.ShapeDtypeStruct((nvar, 1, plevs), jnp.float32),
        ),
        in_specs=[hbm] * 3,
        out_specs=(vmem, vmem, vmem),
        scratch_shapes=[
            pltpu.VMEM((GROUPS, nvar, levels, ROWS, lanes), jnp.bfloat16),
            pltpu.VMEM((GROUPS, plevs, ROWS, lanes), jnp.int32),
            pltpu.VMEM((GROUPS, plevs, ROWS, lanes), jnp.bfloat16),
            pltpu.VMEM((2, planes * 8, lanes), jnp.float32),
            pltpu.VMEM((GROUPS, ROWS, planes, lanes), jnp.bfloat16),
            pltpu.VMEM((8, 8, 1, planes), jnp.float32),
            pltpu.VMEM((8, 8, 1, planes), jnp.float32),
            pltpu.VMEM((8, 1, planes), jnp.float32),
            pltpu.VMEM((24, 1, planes), jnp.float32),
            pltpu.SemaphoreType.DMA((GROUPS, 3)),
            pltpu.SemaphoreType.DMA((GROUPS, 2)),
            pltpu.SemaphoreType.DMA,
            pltpu.SemaphoreType.DMA,
            pltpu.SemaphoreType.DMA,
            pltpu.SemaphoreType.DMA,
            pltpu.SemaphoreType.DMA,
        ],
        compiler_params=pltpu.CompilerParams(
            collective_id=0, has_side_effects=True, vmem_limit_bytes=(64 * 1024 - ROOM_KIB) * 1024
        ),
    )(*args)
    on_pressure, zonal, merid = pl.pallas_call(
        finish,
        name="finish",
        out_shape=(
            jax.ShapeDtypeStruct((planes, PEERS * LANES), jnp.bfloat16),
            jax.ShapeDtypeStruct((nvar, 1, plevs), jnp.float32),
            jax.ShapeDtypeStruct((nvar, 1, plevs), jnp.float32),
        ),
        in_specs=[pl.BlockSpec(memory_space=pl.ANY)] * 3,
        out_specs=(hbm, hbm, hbm),
        scratch_shapes=[pltpu.SemaphoreType.DMA((PIECES + 2,))],
        compiler_params=pltpu.CompilerParams(vmem_limit_bytes=1 * 2**20),
    )(on_pressure, zonal, merid)
    return (
        on_pressure.reshape(nvar, plevs, 1, PEERS * LANES),
        zonal.transpose(0, 2, 1),
        merid.transpose(0, 2, 1),
    )


def solution(mesh):
    finer = Mesh(
        mesh.devices.reshape(4, 2, 4, 2, mesh.shape["lat"]),
        AXES,
    )
    in_specs = (P(None, None, "lat", LON), P(None, "lat", LON), P(None, "lat", LON))
    out_specs = (P(None, None, LAT_LON, None), P(None, None, LAT_LON), P(None, None, LAT_LON))
    return jax.shard_map(
        shards, mesh=finer, in_specs=in_specs, out_specs=out_specs, check_vma=False
    )
```
